32 devices in a mesh: head: 2 (over x), ctx: 16 (over z, y, core).
Axes of the slice: x: 2, y: 2, z: 4, core: 2. Of those that a mesh axis runs over, the one named last changes fastest.
Arguments:
- queries: bfloat16 [8192, 5120], P(('head', 'ctx')), may hold values from -6 to 6
- keys: bfloat16 [8192, 5120], P(('head', 'ctx')), may hold values from -6 to 6
- values: bfloat16 [8192, 5120], P(('head', 'ctx')), may hold values from -6 to 6
- rates: bfloat16 [8192, 8], P(('head', 'ctx')), may hold values from 0.099609375 to 1
- q_gain: float32 [5120], replicated, may hold values from 0.1 to 1.9
- k_gain: float32 [5120], replicated, may hold values from 0.2 to 4.5, as said below
- w_first: float32 [8, 640, 640], P('head'), may hold values from -0.2766993 to 0.2766993
- w_second: float32 [8, 640, 640], P('head'), may hold values from -0.25 to 0.25
- w_third: float32 [8, 640, 640], P('head'), may hold values from -0.2766993 to 0.2766993
Outputs:
- attended: bfloat16 [8192, 5120], P(('head', 'ctx'))
The draws below stay inside these ranges and needn't reach their ends.
Inputs may be any that keep to these rules, and one draw needn't show every extreme that they name: `k_gain`: positive per-feature gains.
All inputs are finite; a program needn't handle non-finite values.
Results may differ from the reference program's by a relative error of at most 0.015.
Values may be sent and summed in bfloat16 or wider, within the bound.
No kernel may reach another device: no remote copies, remote signals or barrier semaphores. Data moves between devices by JAX's collectives and lax.ppermute only.
A program may use at most 128 MiB of HBM per device.

```python
import math
import jax
import jax.numpy as jnp
from jax import lax

HEADS = 8
HD = 640
NS_STEPS = 2
D = 5120
SPAN = 8192


def draw_k_gain(key, part):
    fraction = (jnp.arange(D) % HD).astype(jnp.float32) / HD
    jitter = jax.random.uniform(key, (D,), jnp.float32, 0.8, 1.25)
    return jnp.power(10.0, fraction - 0.5) * jitter


def fast_weight(key):
    fraction = jnp.arange(HD).astype(jnp.float32) / HD
    entries = jnp.clip(jax.random.normal(key, (HEADS, HD, HD), jnp.float32), -3.0, 3.0)
    column = jnp.power(10.0, 0.5 * fraction - 0.25)
    jitter = jax.random.uniform(jax.random.fold_in(key, 7), (HEADS, 1, HD), jnp.float32, 0.8, 1.25)
    return entries * column * jitter / jnp.sqrt(jnp.float32(HD))


def draw_w_first(key, part):
    return fast_weight(jax.random.fold_in(key, 11))


def draw_w_third(key, part):
    return fast_weight(jax.random.fold_in(key, 13))


def steps_of(rng, extent, split, smallest, largest):
    factor_of, own = 1.0, jax.random.fold_in(rng, 6)
    for dim, shards_of in split:
        heights = jnp.exp(jax.random.uniform(jax.random.fold_in(own, dim), (shards_of,), jnp.float32, smallest / len(split), largest / len(split)))
        factor_of = factor_of * jnp.repeat(heights, extent[dim] // shards_of).reshape([-1 if axis == dim else 1 for axis in range(len(extent))])
    return factor_of


def gaussian(key, dims, deviation, reach, split=(), held_as=jnp.bfloat16):
    array = deviation * jax.random.normal(key, dims, jnp.float32)
    if split:
        array = array * steps_of(key, dims, split, -0.22, 0.18)
    return jnp.clip(array, -reach, reach).astype(held_as)


def setup_inputs(seed: int = 0) -> dict:
    key_of = jax.random.split(jax.random.key(seed), 10)
    return {
        "queries": gaussian(key_of[0], (SPAN, D), 1.0, 6.0, ((0, 32),)),
        "keys": gaussian(key_of[1], (SPAN, D), 1.0, 6.0, ((0, 32),)),
        "values": gaussian(key_of[2], (SPAN, D), 1.0, 6.0, ((0, 32),)),
        "rates": jnp.clip(jnp.exp(math.log(1.0) - 2.306499 * jax.random.uniform(key_of[3], (SPAN, HEADS), jnp.float32) ** steps_of(key_of[3], (SPAN, HEADS), ((0, 32),), -0.2, 0.2)), 0.099609375, 1.0).astype(jnp.bfloat16),
        "q_gain": jnp.clip(1.0 + 0.18 * jax.random.normal(key_of[4], (D,), jnp.float32), 0.1, 1.9),
        "k_gain": draw_k_gain(jax.random.fold_in(key_of[9], 71), 0),
        "w_first": draw_w_first(jax.random.fold_in(key_of[9], 71), 0),
        "w_second": gaussian(key_of[7], (HEADS, HD, HD), HD ** -0.5, 0.25, ((0, 2),), jnp.float32),
        "w_third": draw_w_third(jax.random.fold_in(key_of[9], 71), 0),
    }


epsilon = 1e-06
frob_eps = 1e-07
coeff_a = 3.4445
coeff_b = -4.775
coeff_c = 2.0315
step_size = 1.0

def rms_scale(inputs, gain):
    widened = inputs.astype(jnp.float32)
    factor = lax.rsqrt(lax.optimization_barrier(jnp.mean(widened * widened, axis=-1, keepdims=True)) + epsilon)
    return (widened * factor * gain.astype(jnp.float32)).astype(jnp.bfloat16)

def newton_schulz(gradient):
    frob_total = jnp.sqrt(jnp.sum(gradient * gradient))
    iterate = (gradient / (frob_total + frob_eps)).astype(jnp.bfloat16)
    for repeat_index in range(NS_STEPS):
        square = jnp.dot(iterate, iterate.T, preferred_element_type=jnp.float32).astype(jnp.bfloat16)
        polynomial = (coeff_b * square.astype(jnp.float32) + coeff_c * jnp.dot(square, square, preferred_element_type=jnp.float32)).astype(jnp.bfloat16)
        iterate = (coeff_a * iterate.astype(jnp.float32) + jnp.dot(polynomial, iterate, preferred_element_type=jnp.float32)).astype(jnp.bfloat16)
    return iterate

def reference(queries, keys, values, rates, q_gain, k_gain, w_first, w_second, w_third):
    queries_n = rms_scale(queries, q_gain)
    keys_n = rms_scale(keys, k_gain)

    def one_head(head_index):
        start = (head_index * HD).astype(jnp.int32)
        query_block = lax.dynamic_slice_in_dim(queries_n, start, HD, 1)
        key_block = lax.dynamic_slice_in_dim(keys_n, start, HD, 1)
        value_block = lax.dynamic_slice_in_dim(values, start, HD, 1)
        rate_block = lax.dynamic_slice_in_dim(rates, head_index.astype(jnp.int32), 1, 1)
        first = w_first[head_index]
        second = w_second[head_index]
        third = w_third[head_index]
        first_b = first.astype(jnp.bfloat16)
        second_b = second.astype(jnp.bfloat16)
        third_b = third.astype(jnp.bfloat16)
        pre_first = jnp.dot(key_block, first_b, preferred_element_type=jnp.float32)
        pre_third = jnp.dot(key_block, third_b, preferred_element_type=jnp.float32)
        sigmoid = jax.nn.sigmoid(pre_first)
        activ = pre_first * sigmoid
        hidden = (activ * pre_third).astype(jnp.bfloat16)
        scaled_v = (rate_block.astype(jnp.float32) * value_block.astype(jnp.float32)).astype(jnp.bfloat16)
        back_hidden = jnp.dot(scaled_v, second_b.T, preferred_element_type=jnp.float32)
        grad_pre_first = (back_hidden * pre_third * sigmoid * (1.0 + pre_first * (1.0 - sigmoid))).astype(jnp.bfloat16)
        grad_pre_third = (back_hidden * activ).astype(jnp.bfloat16)
        grad_first = jnp.dot(key_block.T, grad_pre_first, preferred_element_type=jnp.float32)
        grad_second = jnp.dot(hidden.T, scaled_v, preferred_element_type=jnp.float32)
        grad_third = jnp.dot(key_block.T, grad_pre_third, preferred_element_type=jnp.float32)
        new_first = (first + step_size * newton_schulz(grad_first).astype(jnp.float32)).astype(jnp.bfloat16)
        new_second = (second + step_size * newton_schulz(grad_second).astype(jnp.float32)).astype(jnp.bfloat16)
        new_third = (third + step_size * newton_schulz(grad_third).astype(jnp.float32)).astype(jnp.bfloat16)
        query_first = jnp.dot(query_block, new_first, preferred_element_type=jnp.float32)
        query_third = jnp.dot(query_block, new_third, preferred_element_type=jnp.float32)
        gated = (jax.nn.silu(query_first) * query_third).astype(jnp.bfloat16)
        result = jnp.dot(gated, new_second, preferred_element_type=jnp.float32)
        factor = lax.rsqrt(lax.optimization_barrier(jnp.mean(result * result, axis=-1, keepdims=True)) + epsilon)
        return (result * factor).astype(jnp.bfloat16)
    blocks = lax.map(one_head, jnp.arange(HEADS, dtype=jnp.int32))
    return jnp.transpose(blocks, (1, 0, 2)).reshape(SPAN, HEADS * HD)
```

```python
import functools

import jax
import jax.numpy as jnp
from jax import lax
from jax.experimental import pallas as pl
from jax.experimental.pallas import tpu as pltpu
from jax.sharding import Mesh, PartitionSpec as P


NS_STEPS = 2

epsilon = 1e-06
frob_eps = 1e-07
coeff_a = 3.4445
coeff_b = -4.775
coeff_c = 2.0315
step_size = 1.0

f32 = jnp.float32
bf16 = jnp.bfloat16
NT = (((1,), (1,)), ((), ()))


def mm(a, b):
    return jnp.dot(a, b, preferred_element_type=f32)


def cost(flops, moved):
    return pl.CostEstimate(flops=flops, bytes_accessed=moved, transcendentals=0)


def normalized(x_ref, gain_ref, out_ref, place):
    heads, width = out_ref.shape[0], out_ref.shape[-1]
    wide = x_ref[...].astype(f32)
    factor = lax.rsqrt(jnp.mean(wide * wide, axis=-1, keepdims=True) + epsilon)
    for head in range(heads):
        cols = slice(head * width, (head + 1) * width)
        out_ref[place(head)] = (
            x_ref[:, cols].astype(f32) * factor * gain_ref[:, cols]
        ).astype(bf16)


def query_kernel(x_ref, gain_ref, out_ref):
    normalized(x_ref, gain_ref, out_ref, lambda head: head)


def pair_kernel(k_ref, v_ref, rate_ref, gain_ref, out_ref):
    heads, width = out_ref.shape[0], out_ref.shape[-1]
    normalized(k_ref, gain_ref, out_ref, lambda head: (head, 0))
    for head in range(heads):
        cols = slice(head * width, (head + 1) * width)
        rate = rate_ref[:, head : head + 1].astype(f32)
        out_ref[head, 1] = (v_ref[:, cols].astype(f32) * rate).astype(bf16)


def prepared_queries(x, gain, heads):
    rows, model = x.shape
    width = model // heads
    block = rows // 4 if rows % 64 == 0 else rows
    return pl.pallas_call(
        query_kernel,
        grid=(rows // block,),
        in_specs=[
            pl.BlockSpec((block, model), lambda i: (i, 0)),
            pl.BlockSpec((1, model), lambda i: (0, 0)),
        ],
        out_specs=pl.BlockSpec((heads, block, width), lambda i: (0, i, 0)),
        out_shape=jax.ShapeDtypeStruct((heads, rows, width), bf16),
        cost_estimate=cost(8 * rows * model, 4 * rows * model),
    )(x, gain)


def prepared_pair(keys, values, rates, gain, first, steps, block):
    heads = rates.shape[1]
    model = keys.shape[1]
    rows = block * steps
    width = model // heads
    tile = pl.BlockSpec((block, model), lambda i: (first + i, 0))
    return pl.pallas_call(
        pair_kernel,
        grid=(steps,),
        in_specs=[
            tile,
            tile,
            pl.BlockSpec((block, heads), lambda i: (first + i, 0)),
            pl.BlockSpec((1, model), lambda i: (0, 0)),
        ],
        out_specs=pl.BlockSpec((heads, 2, block, width), lambda i: (0, 0, i, 0)),
        out_shape=jax.ShapeDtypeStruct((heads, 2, rows, width), bf16),
        cost_estimate=cost(12 * rows * model, 8 * rows * model),
    )(keys, values, rates, gain)


def back_to_columns(x):
    heads, rows, width = x.shape

    def kernel(x_ref, out_ref):
        for head in range(heads):
            out_ref[:, head * width : (head + 1) * width] = x_ref[head]

    block = rows // 4 if rows % 64 == 0 else rows
    return pl.pallas_call(
        kernel,
        grid=(rows // block,),
        in_specs=[pl.BlockSpec((heads, block, width), lambda i: (0, i, 0))],
        out_specs=pl.BlockSpec((block, heads * width), lambda i: (i, 0)),
        out_shape=jax.ShapeDtypeStruct((rows, heads * width), bf16),
        cost_estimate=cost(rows * heads * width, 4 * rows * heads * width),
    )(x)


def accumulate(pair_ref, wb1, wb2, wb3, acc1, acc2, acc3):
    sources, _, rows, width = pair_ref.shape
    keys = pair_ref[:, 0].reshape(sources * rows, width)
    scaled = pair_ref[:, 1].reshape(sources * rows, width)
    pre1 = mm(keys, wb1[...])
    pre3 = mm(keys, wb3[...])
    sigmoid = jax.nn.sigmoid(pre1)
    activ = pre1 * sigmoid
    hidden = (activ * pre3).astype(bf16)
    back = mm(scaled, wb2[...])
    d1 = (back * pre3 * sigmoid * (1.0 + pre1 * (1.0 - sigmoid))).astype(bf16)
    d3 = (back * activ).astype(bf16)
    keys_t = keys.T
    acc1[...] += mm(keys_t, d1)
    acc3[...] += mm(keys_t, d3)
    acc2[...] += mm(hidden.T, scaled)


def first_kernel(
    ids, pair_ref, w1_ref, w2_ref, w3_ref, acc1, acc2, acc3, wb1, wb2, wb3
):
    @pl.when(pl.program_id(0) == 0)
    def _():
        wb1[...] = w1_ref[0].astype(bf16)
        wb2[...] = w2_ref[0].astype(bf16).T
        wb3[...] = w3_ref[0].astype(bf16)
        for acc in (acc1, acc2, acc3):
            acc[...] = jnp.zeros_like(acc)

    accumulate(pair_ref, wb1, wb2, wb3, acc1, acc2, acc3)


def last_kernel(
    ids, pair_ref, was1, was2, was3, wb1, wb2, wb3,
    send1, keep1, send2, keep2, send3, keep3, acc1, acc2, acc3,
):
    @pl.when(pl.program_id(0) == 0)
    def _():
        for acc in (acc1, acc2, acc3):
            acc[...] = jnp.zeros_like(acc)

    accumulate(pair_ref, wb1, wb2, wb3, acc1, acc2, acc3)

    @pl.when(pl.program_id(0) == pl.num_programs(0) - 1)
    def _():
        half = keep1.shape[0]
        mine = pl.ds(pl.multiple_of(ids[1] * half, 16), half)
        other = pl.ds(pl.multiple_of((1 - ids[1]) * half, 16), half)
        for was, acc, send, keep in (
            (was1, acc1, send1, keep1),
            (was2, acc2, send2, keep2),
            (was3, acc3, send3, keep3),
        ):
            send[...] = (was[other, :] + acc[other, :]).astype(bf16)
            keep[...] = was[mine, :] + acc[mine, :]


def grad_call(kernel, ids, pair, others, other_specs, outs, out_specs, scratch):
    heads, _, rows, width = pair.shape
    sources = heads // 2 if heads % 2 == 0 else heads
    return pl.pallas_call(
        kernel,
        grid_spec=pltpu.PrefetchScalarGridSpec(
            num_scalar_prefetch=1,
            grid=(heads // sources,),
            in_specs=[pl.BlockSpec((sources, 2, rows, width), lambda i, ids: (i, 0, 0, 0))]
            + other_specs,
            out_specs=out_specs,
            scratch_shapes=scratch,
        ),
        out_shape=outs,
        cost_estimate=cost(12 * heads * rows * width * width, 4 * heads * rows * width),
        compiler_params=pltpu.CompilerParams(vmem_limit_bytes=60 << 20),
    )(ids, pair, *others)


def gradients_first(ids, pair, weights):
    width = pair.shape[-1]
    weight = pl.BlockSpec((1, width, width), lambda i, ids: (ids[0], 0, 0))
    full = pl.BlockSpec((width, width), lambda i, ids: (0, 0))
    outs = [jax.ShapeDtypeStruct((width, width), f32)] * 3
    outs += [jax.ShapeDtypeStruct((width, width), bf16)] * 3
    return grad_call(first_kernel, ids, pair, weights, [weight] * 3, outs, [full] * 6, [])


def gradients_last(ids, pair, carried):
    width = pair.shape[-1]
    rows = width // 2
    full = pl.BlockSpec((width, width), lambda i, ids: (0, 0))
    half = pl.BlockSpec((rows, width), lambda i, ids: (0, 0))
    outs = [
        jax.ShapeDtypeStruct((rows, width), bf16),
        jax.ShapeDtypeStruct((rows, width), f32),
    ] * 3
    scratch = [pltpu.VMEM((width, width), f32)] * 3
    return grad_call(last_kernel, ids, pair, carried, [full] * 6, outs, [half] * 6, scratch)


def newton_kernel(ids, g_ref, w_ref, u_ref):
    grad = g_ref[...].astype(f32)
    total = jnp.sqrt(jnp.sum(grad * grad))
    x = (grad / (total + frob_eps)).astype(bf16)
    for _ in range(NS_STEPS):
        square = lax.dot_general(x, x, NT, preferred_element_type=f32).astype(bf16)
        poly = (coeff_b * square.astype(f32) + coeff_c * mm(square, square)).astype(bf16)
        x = (coeff_a * x.astype(f32) + mm(poly, x)).astype(bf16)
    u_ref[...] = (w_ref[0] + step_size * x.astype(f32)).astype(bf16)


def updated(ids, grad, weight):
    width = grad.shape[0]
    full = pl.BlockSpec((width, width), lambda i, ids: (0, 0))
    return pl.pallas_call(
        newton_kernel,
        grid_spec=pltpu.PrefetchScalarGridSpec(
            num_scalar_prefetch=1,
            grid=(1,),
            in_specs=[full, pl.BlockSpec((1, width, width), lambda i, ids: (ids[0], 0, 0))],
            out_specs=full,
        ),
        out_shape=jax.ShapeDtypeStruct((width, width), bf16),
        cost_estimate=cost(12 * width**3, 8 * width * width),
        compiler_params=pltpu.CompilerParams(vmem_limit_bytes=60 << 20),
    )(ids, grad, weight)


def gate_kernel(q_ref, u1_ref, u3_ref, f_ref):
    pre1 = mm(q_ref[...], u1_ref[...])
    pre3 = mm(q_ref[...], u3_ref[...])
    f_ref[...] = (pre1 * jax.nn.sigmoid(pre1) * pre3).astype(bf16)


def output_kernel(f_ref, u2_ref, o_ref):
    out = mm(f_ref[...], u2_ref[...])
    factor = lax.rsqrt(jnp.mean(out * out, axis=-1, keepdims=True) + epsilon)
    o_ref[...] = (out * factor).astype(bf16)


def over_tokens(kernel, x, *weights):
    tokens, width = x.shape
    block = tokens // 4
    tile = pl.BlockSpec((block, width), lambda i: (i, 0))
    full = pl.BlockSpec((width, width), lambda i: (0, 0))
    return pl.pallas_call(
        kernel,
        grid=(tokens // block,),
        in_specs=[tile] + [full] * len(weights),
        out_specs=tile,
        out_shape=jax.ShapeDtypeStruct((tokens, width), bf16),
        cost_estimate=cost(2 * len(weights) * tokens * width * width, 4 * tokens * width),
        compiler_params=pltpu.CompilerParams(vmem_limit_bytes=60 << 20),
    )(x, *weights)


def summed(send, keep, steps):
    for place, (axis, size, bit) in enumerate(steps):
        pairs = [(i, i ^ (1 << bit)) for i in range(size)]
        came = lax.ppermute(send, axis, pairs)
        keep = keep + came.astype(f32)
        if place + 1 == len(steps):
            whole = keep.astype(bf16)
            break
        axis, size, bit = steps[place + 1]
        rows = keep.shape[0] // 2
        side = (lax.axis_index(axis) >> bit) & 1
        send = lax.dynamic_slice_in_dim(keep, (1 - side) * rows, rows, 0).astype(bf16)
        keep = lax.dynamic_slice_in_dim(keep, side * rows, rows, 0)
    for place, (axis, size, bit) in reversed(list(enumerate(steps))):
        pairs = [(i, i ^ (1 << bit)) for i in range(size)]
        other = lax.ppermute(whole, axis, pairs)
        first = ((lax.axis_index(axis) >> bit) & 1) == 0
        whole = jnp.concatenate(
            [jnp.where(first, whole, other), jnp.where(first, other, whole)], axis=0
        )
    return whole


def per_device(
    sizes, queries, keys, values, rates, q_gain, k_gain, w_first, w_second, w_third
):
    heads = rates.shape[1]
    width = w_first.shape[1]
    exchange = functools.partial(
        lax.all_to_all, axis_name=("head", "l1", "l2"), split_axis=0, concat_axis=0, tiled=True
    )
    steps = [
        (axis, sizes[axis], bit)
        for axis in ("h2", "h1")
        for bit in range(sizes[axis].bit_length() - 1)
    ]
    axis, _, bit = steps[0]
    ids = jnp.stack([
        lax.axis_index("l1") * sizes["l2"] + lax.axis_index("l2"),
        (lax.axis_index(axis) >> bit) & 1,
    ]).astype(jnp.int32)
    pairs = []
    block = keys.shape[0] // 4
    for start, count in ((0, 3), (3, 1)):
        pair = prepared_pair(keys, values, rates, k_gain[None], start, count, block)
        pairs.append(exchange(pair))
    ready = prepared_queries(queries, q_gain[None], heads)
    query_local = exchange(ready)
    carried = gradients_first(ids, pairs[0], (w_first, w_second, w_third))
    s1, p1, s2, p2, s3, p3 = gradients_last(ids, pairs[1], carried)
    full_first = summed(s1, p1, steps)
    full_third = summed(s3, p3, steps)
    full_second = summed(s2, p2, steps)
    new_first = updated(ids, full_first, w_first)
    new_third = updated(ids, full_third, w_third)
    gated = over_tokens(gate_kernel, query_local.reshape(-1, width), new_first, new_third)
    new_second = updated(ids, full_second, w_second)
    normed = over_tokens(output_kernel, gated, new_second)
    return back_to_columns(exchange(normed.reshape(heads, -1, width)))


def solution(mesh):
    head, ctx = mesh.shape["head"], mesh.shape["ctx"]

    def run(queries, keys, values, rates, q_gain, k_gain, w_first, w_second, w_third):
        lo = w_first.shape[0] // head
        hi = ctx // lo
        sizes = {"l2": min(lo, 2), "h2": min(hi, 2)}
        sizes["l1"] = lo // sizes["l2"]
        sizes["h1"] = hi // sizes["h2"]
        assert hi > 1 and hi * lo == ctx and ctx & (ctx - 1) == 0
        assert w_first.shape[1] % (2 * hi) == 0
        order = ("h1", "l1", "h2", "l2")
        shape = [head] + [sizes[axis] for axis in order]
        inner = Mesh(mesh.devices.reshape(shape), ("head",) + order)
        tokens = P(("head",) + order, None)
        return jax.shard_map(
            functools.partial(per_device, sizes),
            mesh=inner,
            in_specs=(tokens,) * 4 + (P(), P()) + (P("head", None, None),) * 3,
            out_specs=tokens,
            check_vma=False,
        )(queries, keys, values, rates, q_gain, k_gain, w_first, w_second, w_third)

    return run
```

```python
import functools

import jax
import jax.numpy as jnp
from jax import lax
from jax.experimental import pallas as pl
from jax.experimental.pallas import tpu as pltpu
from jax.sharding import Mesh, PartitionSpec as P


NS_STEPS = 2

epsilon = 1e-06
frob_eps = 1e-07
coeff_a = 3.4445
coeff_b = -4.775
coeff_c = 2.0315
step_size = 1.0

f32 = jnp.float32
bf16 = jnp.bfloat16
NT = (((1,), (1,)), ((), ()))


def mm(a, b):
    return jnp.dot(a, b, preferred_element_type=f32)


def cost(flops, moved):
    return pl.CostEstimate(flops=flops, bytes_accessed=moved, transcendentals=0)


def normalized(x_ref, gain_ref, out_ref, place):
    heads, width = out_ref.shape[0], out_ref.shape[-1]
    wide = x_ref[...].astype(f32)
    factor = lax.rsqrt(jnp.mean(wide * wide, axis=-1, keepdims=True) + epsilon)
    for head in range(heads):
        cols = slice(head * width, (head + 1) * width)
        out_ref[place(head)] = (
            x_ref[:, cols].astype(f32) * factor * gain_ref[:, cols]
        ).astype(bf16)


def query_kernel(x_ref, gain_ref, out_ref):
    normalized(x_ref, gain_ref, out_ref, lambda head: head)


def pair_kernel(k_ref, v_ref, rate_ref, gain_ref, out_ref):
    heads, width = out_ref.shape[0], out_ref.shape[-1]
    normalized(k_ref, gain_ref, out_ref, lambda head: (head, 0))
    for head in range(heads):
        cols = slice(head * width, (head + 1) * width)
        rate = rate_ref[:, head : head + 1].astype(f32)
        out_ref[head, 1] = (v_ref[:, cols].astype(f32) * rate).astype(bf16)


def prepared_queries(x, gain, heads):
    rows, model = x.shape
    width = model // heads
    block = rows // 4 if rows % 64 == 0 else rows
    return pl.pallas_call(
        query_kernel,
        grid=(rows // block,),
        in_specs=[
            pl.BlockSpec((block, model), lambda i: (i, 0)),
            pl.BlockSpec((1, model), lambda i: (0, 0)),
        ],
        out_specs=pl.BlockSpec((heads, block, width), lambda i: (0, i, 0)),
        out_shape=jax.ShapeDtypeStruct((heads, rows, width), bf16),
        cost_estimate=cost(8 * rows * model, 4 * rows * model),
    )(x, gain)


def prepared_pair(keys, values, rates, gain, first, steps, block):
    heads = rates.shape[1]
    model = keys.shape[1]
    rows = block * steps
    width = model // heads
    tile = pl.BlockSpec((block, model), lambda i: (first + i, 0))
    return pl.pallas_call(
        pair_kernel,
        grid=(steps,),
        in_specs=[
            tile,
            tile,
            pl.BlockSpec((block, heads), lambda i: (first + i, 0)),
            pl.BlockSpec((1, model), lambda i: (0, 0)),
        ],
        out_specs=pl.BlockSpec((heads, 2, block, width), lambda i: (0, 0, i, 0)),
        out_shape=jax.ShapeDtypeStruct((heads, 2, rows, width), bf16),
        cost_estimate=cost(12 * rows * model, 8 * rows * model),
    )(keys, values, rates, gain)


def back_to_columns(x):
    heads, rows, width = x.shape

    def kernel(x_ref, out_ref):
        for head in range(heads):
            out_ref[:, head * width : (head + 1) * width] = x_ref[head]

    block = rows // 4 if rows % 64 == 0 else rows
    return pl.pallas_call(
        kernel,
        grid=(rows // block,),
        in_specs=[pl.BlockSpec((heads, block, width), lambda i: (0, i, 0))],
        out_specs=pl.BlockSpec((block, heads * width), lambda i: (i, 0)),
        out_shape=jax.ShapeDtypeStruct((rows, heads * width), bf16),
        cost_estimate=cost(rows * heads * width, 4 * rows * heads * width),
    )(x)


def accumulate(pair_ref, wb1, wb2, wb3, acc1, acc2, acc3):
    sources, _, rows, width = pair_ref.shape
    keys = pair_ref[:, 0].reshape(sources * rows, width)
    scaled = pair_ref[:, 1].reshape(sources * rows, width)
    pre1 = mm(keys, wb1[...])
    pre3 = mm(keys, wb3[...])
    sigmoid = jax.nn.sigmoid(pre1)
    activ = pre1 * sigmoid
    hidden = (activ * pre3).astype(bf16)
    back = mm(scaled, wb2[...])
    d1 = (back * pre3 * sigmoid * (1.0 + pre1 * (1.0 - sigmoid))).astype(bf16)
    d3 = (back * activ).astype(bf16)
    keys_t = keys.T
    acc1[...] += mm(keys_t, d1)
    acc3[...] += mm(keys_t, d3)
    acc2[...] += mm(hidden.T, scaled)


def first_kernel(
    ids, pair_ref, w1_ref, w2_ref, w3_ref, acc1, acc2, acc3, wb1, wb2, wb3
):
    @pl.when(pl.program_id(0) == 0)
    def _():
        wb1[...] = w1_ref[0].astype(bf16)
        wb2[...] = w2_ref[0].astype(bf16).T
        wb3[...] = w3_ref[0].astype(bf16)
        for acc in (acc1, acc2, acc3):
            acc[...] = jnp.zeros_like(acc)

    accumulate(pair_ref, wb1, wb2, wb3, acc1, acc2, acc3)


def last_kernel(
    ids, pair_ref, was1, was2, was3, wb1, wb2, wb3,
    send1, keep1, send2, keep2, send3, keep3, acc1, acc2, acc3, old1, old2, old3, sems,
):
    loads = [
        pltpu.make_async_copy(was, old, sems.at[i])
        for i, (was, old) in enumerate(((was1, old1), (was2, old2), (was3, old3)))
    ]

    @pl.when(pl.program_id(0) == 0)
    def _():
        for load in loads:
            load.start()
        for acc in (acc1, acc2, acc3):
            acc[...] = jnp.zeros_like(acc)

    accumulate(pair_ref, wb1, wb2, wb3, acc1, acc2, acc3)

    @pl.when(pl.program_id(0) == pl.num_programs(0) - 1)
    def _():
        half = keep1.shape[0]
        mine = pl.ds(pl.multiple_of(ids[1] * half, 16), half)
        other = pl.ds(pl.multiple_of((1 - ids[1]) * half, 16), half)
        for load, was, acc, send, keep in (
            (loads[0], old1, acc1, send1, keep1),
            (loads[2], old3, acc3, send3, keep3),
            (loads[1], old2, acc2, send2, keep2),
        ):
            load.wait()
            send[...] = (was[other, :] + acc[other, :]).astype(bf16)
            keep[...] = was[mine, :] + acc[mine, :]


def grad_call(kernel, ids, pair, others, other_specs, outs, out_specs, scratch):
    heads, _, rows, width = pair.shape
    sources = heads // 2 if heads % 2 == 0 else heads
    return pl.pallas_call(
        kernel,
        grid_spec=pltpu.PrefetchScalarGridSpec(
            num_scalar_prefetch=1,
            grid=(heads // sources,),
            in_specs=[pl.BlockSpec((sources, 2, rows, width), lambda i, ids: (i, 0, 0, 0))]
            + other_specs,
            out_specs=out_specs,
            scratch_shapes=scratch,
        ),
        out_shape=outs,
        cost_estimate=cost(12 * heads * rows * width * width, 4 * heads * rows * width),
        compiler_params=pltpu.CompilerParams(vmem_limit_bytes=60 << 20),
    )(ids, pair, *others)


def gradients_first(ids, pair, weights):
    width = pair.shape[-1]
    weight = pl.BlockSpec((1, width, width), lambda i, ids: (ids[0], 0, 0))
    full = pl.BlockSpec((width, width), lambda i, ids: (0, 0))
    outs = [jax.ShapeDtypeStruct((width, width), f32)] * 3
    outs += [jax.ShapeDtypeStruct((width, width), bf16)] * 3
    return grad_call(first_kernel, ids, pair, weights, [weight] * 3, outs, [full] * 6, [])


def gradients_last(ids, pair, carried):
    width = pair.shape[-1]
    rows = width // 2
    full = pl.BlockSpec((width, width), lambda i, ids: (0, 0))
    half = pl.BlockSpec((rows, width), lambda i, ids: (0, 0))
    outs = [
        jax.ShapeDtypeStruct((rows, width), bf16),
        jax.ShapeDtypeStruct((rows, width), f32),
    ] * 3
    scratch = [pltpu.VMEM((width, width), f32)] * 6 + [pltpu.SemaphoreType.DMA((3,))]
    specs = [pl.BlockSpec(memory_space=pl.ANY)] * 3 + [full] * 3
    return grad_call(last_kernel, ids, pair, carried, specs, outs, [half] * 6, scratch)


def newton_kernel(ids, own_ref, other_ref, w_ref, u_ref, g_ref):
    half = own_ref.shape[0]
    g_ref[pl.ds(pl.multiple_of(ids[1] * half, 16), half), :] = own_ref[...]
    g_ref[pl.ds(pl.multiple_of((1 - ids[1]) * half, 16), half), :] = other_ref[...]
    grad = g_ref[...].astype(f32)
    total = jnp.sqrt(jnp.sum(grad * grad))
    x = (grad / (total + frob_eps)).astype(bf16)
    for _ in range(NS_STEPS):
        square = lax.dot_general(x, x, NT, preferred_element_type=f32).astype(bf16)
        poly = (coeff_b * square.astype(f32) + coeff_c * mm(square, square)).astype(bf16)
        x = (coeff_a * x.astype(f32) + mm(poly, x)).astype(bf16)
    u_ref[...] = (w_ref[0] + step_size * x.astype(f32)).astype(bf16)


def updated(ids, halves, weight):
    rows, width = halves[0].shape
    half = pl.BlockSpec((rows, width), lambda i, ids: (0, 0))
    full = pl.BlockSpec((width, width), lambda i, ids: (0, 0))
    return pl.pallas_call(
        newton_kernel,
        grid_spec=pltpu.PrefetchScalarGridSpec(
            num_scalar_prefetch=1,
            grid=(1,),
            in_specs=[half, half, pl.BlockSpec((1, width, width), lambda i, ids: (ids[0], 0, 0))],
            out_specs=full,
            scratch_shapes=[pltpu.VMEM((width, width), bf16)],
        ),
        out_shape=jax.ShapeDtypeStruct((width, width), bf16),
        cost_estimate=cost(12 * width**3, 8 * width * width),
        compiler_params=pltpu.CompilerParams(vmem_limit_bytes=60 << 20),
    )(ids, *halves, weight)


def gate_kernel(q_ref, u1_ref, u3_ref, f_ref):
    pre1 = mm(q_ref[...], u1_ref[...])
    pre3 = mm(q_ref[...], u3_ref[...])
    f_ref[...] = (pre1 * jax.nn.sigmoid(pre1) * pre3).astype(bf16)


def output_kernel(f_ref, u2_ref, o_ref):
    out = mm(f_ref[...], u2_ref[...])
    factor = lax.rsqrt(jnp.mean(out * out, axis=-1, keepdims=True) + epsilon)
    o_ref[...] = (out * factor).astype(bf16)


def over_tokens(kernel, x, *weights):
    tokens, width = x.shape
    block = tokens // 4
    tile = pl.BlockSpec((block, width), lambda i: (i, 0))
    full = pl.BlockSpec((width, width), lambda i: (0, 0))
    return pl.pallas_call(
        kernel,
        grid=(tokens // block,),
        in_specs=[tile] + [full] * len(weights),
        out_specs=tile,
        out_shape=jax.ShapeDtypeStruct((tokens, width), bf16),
        cost_estimate=cost(2 * len(weights) * tokens * width * width, 4 * tokens * width),
        compiler_params=pltpu.CompilerParams(vmem_limit_bytes=60 << 20),
    )(x, *weights)


def summed(send, keep, steps):
    for place, (axis, size, bit) in enumerate(steps):
        pairs = [(i, i ^ (1 << bit)) for i in range(size)]
        came = lax.ppermute(send, axis, pairs)
        keep = keep + came.astype(f32)
        if place + 1 == len(steps):
            whole = keep.astype(bf16)
        elif place + 2 == len(steps):
            send = keep.astype(bf16)
        else:
            axis, size, bit = steps[place + 1]
            rows = keep.shape[0] // 2
            side = (lax.axis_index(axis) >> bit) & 1
            send = lax.dynamic_slice_in_dim(keep, (1 - side) * rows, rows, 0).astype(bf16)
            keep = lax.dynamic_slice_in_dim(keep, side * rows, rows, 0)
    for place, (axis, size, bit) in reversed(list(enumerate(steps[:-1]))):
        pairs = [(i, i ^ (1 << bit)) for i in range(size)]
        other = lax.ppermute(whole, axis, pairs)
        if place == 0:
            return whole, other
        first = ((lax.axis_index(axis) >> bit) & 1) == 0
        whole = jnp.concatenate(
            [jnp.where(first, whole, other), jnp.where(first, other, whole)], axis=0
        )


def per_device(
    sizes, queries, keys, values, rates, q_gain, k_gain, w_first, w_second, w_third
):
    heads = rates.shape[1]
    width = w_first.shape[1]
    exchange = functools.partial(
        lax.all_to_all, axis_name=("head", "l1", "l2"), split_axis=0, concat_axis=0, tiled=True
    )
    steps = [
        (axis, sizes[axis], bit)
        for axis in ("h2", "h1")
        for bit in range(sizes[axis].bit_length() - 1)
    ]
    axis, _, bit = steps[0]
    ids = jnp.stack([
        lax.axis_index("l1") * sizes["l2"] + lax.axis_index("l2"),
        (lax.axis_index(axis) >> bit) & 1,
    ]).astype(jnp.int32)
    pairs = []
    block = keys.shape[0] // 4
    for start, count in ((0, 3), (3, 1)):
        pair = prepared_pair(keys, values, rates, k_gain[None], start, count, block)
        pairs.append(exchange(pair))
    ready = prepared_queries(queries, q_gain[None], heads)
    query_local = exchange(ready)
    carried = gradients_first(ids, pairs[0], (w_first, w_second, w_third))
    s1, p1, s2, p2, s3, p3 = gradients_last(ids, pairs[1], carried)
    full_first = summed(s1, p1, steps)
    full_third = summed(s3, p3, steps)
    full_second = summed(s2, p2, steps)
    new_first = updated(ids, full_first, w_first)
    new_third = updated(ids, full_third, w_third)
    gated = over_tokens(gate_kernel, query_local.reshape(-1, width), new_first, new_third)
    new_second = updated(ids, full_second, w_second)
    normed = over_tokens(output_kernel, gated, new_second)
    return back_to_columns(exchange(normed.reshape(heads, -1, width)))


def solution(mesh):
    head, ctx = mesh.shape["head"], mesh.shape["ctx"]

    def run(queries, keys, values, rates, q_gain, k_gain, w_first, w_second, w_third):
        lo = w_first.shape[0] // head
        hi = ctx // lo
        sizes = {"l2": min(lo, 2), "h2": min(hi, 2)}
        sizes["l1"] = lo // sizes["l2"]
        sizes["h1"] = hi // sizes["h2"]
        assert hi > 2 and hi * lo == ctx and ctx & (ctx - 1) == 0
        assert w_first.shape[1] % (2 * hi) == 0
        order = ("h1", "l1", "h2", "l2")
        shape = [head] + [sizes[axis] for axis in order]
        inner = Mesh(mesh.devices.reshape(shape), ("head",) + order)
        tokens = P(("head",) + order, None)
        return jax.shard_map(
            functools.partial(per_device, sizes),
            mesh=inner,
            in_specs=(tokens,) * 4 + (P(), P()) + (P("head", None, None),) * 3,
            out_specs=tokens,
            check_vma=False,
        )(queries, keys, values, rates, q_gain, k_gain, w_first, w_second, w_third)

    return run
```

```python
import functools

import jax
import jax.numpy as jnp
from jax import lax
from jax.experimental import pallas as pl
from jax.experimental.pallas import tpu as pltpu
from jax.sharding import Mesh, PartitionSpec as P


NS_STEPS = 2

epsilon = 1e-06
frob_eps = 1e-07
coeff_a = 3.4445
coeff_b = -4.775
coeff_c = 2.0315
step_size = 1.0

f32 = jnp.float32
bf16 = jnp.bfloat16
NT = (((1,), (1,)), ((), ()))


def mm(a, b):
    return jnp.dot(a, b, preferred_element_type=f32)


def cost(flops, moved):
    return pl.CostEstimate(flops=flops, bytes_accessed=moved, transcendentals=0)


def normalized(x_ref, gain_ref, out_ref, place):
    heads, width = out_ref.shape[0], out_ref.shape[-1]
    wide = x_ref[...].astype(f32)
    factor = lax.rsqrt(jnp.mean(wide * wide, axis=-1, keepdims=True) + epsilon)
    for head in range(heads):
        cols = slice(head * width, (head + 1) * width)
        out_ref[place(head)] = (
            x_ref[:, cols].astype(f32) * factor * gain_ref[:, cols]
        ).astype(bf16)


def query_kernel(x_ref, gain_ref, out_ref):
    normalized(x_ref, gain_ref, out_ref, lambda head: head)


def pair_kernel(ids, k_ref, v_ref, rate_ref, gain_ref, *out_refs):
    width = out_refs[0].shape[-1]
    wide = k_ref[...].astype(f32)
    factor = lax.rsqrt(jnp.mean(wide * wide, axis=-1, keepdims=True) + epsilon)
    rates = rate_ref[...].astype(f32)
    lane = lax.broadcasted_iota(jnp.int32, rates.shape, 1)
    for k, out_ref in enumerate(out_refs):
        head = ids[2] ^ k
        cols = pl.ds(pl.multiple_of(head * width, 128), width)
        out_ref[0] = (k_ref[:, cols].astype(f32) * factor * gain_ref[:, cols]).astype(bf16)
        rate = jnp.sum(jnp.where(lane == head, rates, 0.0), axis=1, keepdims=True)
        out_ref[1] = (v_ref[:, cols].astype(f32) * rate).astype(bf16)


def prepared_queries(x, gain, heads):
    rows, model = x.shape
    width = model // heads
    block = rows // 4 if rows % 64 == 0 else rows
    return pl.pallas_call(
        query_kernel,
        grid=(rows // block,),
        in_specs=[
            pl.BlockSpec((block, model), lambda i: (i, 0)),
            pl.BlockSpec((1, model), lambda i: (0, 0)),
        ],
        out_specs=pl.BlockSpec((heads, block, width), lambda i: (0, i, 0)),
        out_shape=jax.ShapeDtypeStruct((heads, rows, width), bf16),
        cost_estimate=cost(8 * rows * model, 4 * rows * model),
    )(x, gain)


def prepared_pair(ids, keys, values, rates, gain, first, steps, block):
    heads = rates.shape[1]
    model = keys.shape[1]
    rows = block * steps
    width = model // heads
    tile = pl.BlockSpec((block, model), lambda i, ids: (first + i, 0))
    return pl.pallas_call(
        pair_kernel,
        grid_spec=pltpu.PrefetchScalarGridSpec(
            num_scalar_prefetch=1,
            grid=(steps,),
            in_specs=[
                tile,
                tile,
                pl.BlockSpec((block, heads), lambda i, ids: (first + i, 0)),
                pl.BlockSpec((1, model), lambda i, ids: (0, 0)),
            ],
            out_specs=[pl.BlockSpec((2, block, width), lambda i, ids: (0, i, 0))] * heads,
        ),
        out_shape=[jax.ShapeDtypeStruct((2, rows, width), bf16)] * heads,
        cost_estimate=cost(12 * rows * model, 8 * rows * model),
    )(ids, keys, values, rates, gain)


def back_to_columns(ids, blocks):
    rows, width = blocks[0].shape
    heads = len(blocks)

    def kernel(ids, *refs):
        out_ref = refs[-1]
        for k, ref in enumerate(refs[:-1]):
            start = pl.multiple_of((ids[2] ^ k) * width, 128)
            out_ref[:, pl.ds(start, width)] = ref[...]

    block = rows // 4
    return pl.pallas_call(
        kernel,
        grid_spec=pltpu.PrefetchScalarGridSpec(
            num_scalar_prefetch=1,
            grid=(rows // block,),
            in_specs=[pl.BlockSpec((block, width), lambda i, ids: (i, 0))] * heads,
            out_specs=pl.BlockSpec((block, heads * width), lambda i, ids: (i, 0)),
        ),
        out_shape=jax.ShapeDtypeStruct((rows, heads * width), bf16),
        cost_estimate=cost(rows * heads * width, 4 * rows * heads * width),
    )(ids, *blocks)


def fetch(pair_refs, buffer, sems):
    loads = [
        pltpu.make_async_copy(ref, buffer.at[i], sems.at[i]) for i, ref in enumerate(pair_refs)
    ]
    half = len(loads) // 2

    @pl.when(pl.program_id(0) == 0)
    def _():
        for load in loads:
            load.start()

    return loads[:half], loads[half:]


def accumulate(groups, buffer, wb1, wb2, wb3, acc1, acc2, acc3):
    for step, group in enumerate(groups):

        @pl.when(pl.program_id(0) == step)
        def _():
            for load in group:
                load.wait()

    sources, rows, width = buffer.shape[0] // 2, buffer.shape[2], buffer.shape[3]
    now = pl.ds(pl.program_id(0) * sources, sources)
    keys = buffer[now, 0].reshape(sources * rows, width)
    scaled = buffer[now, 1].reshape(sources * rows, width)
    pre1 = mm(keys, wb1[...])
    pre3 = mm(keys, wb3[...])
    sigmoid = jax.nn.sigmoid(pre1)
    activ = pre1 * sigmoid
    hidden = (activ * pre3).astype(bf16)
    back = mm(scaled, wb2[...])
    d1 = (back * pre3 * sigmoid * (1.0 + pre1 * (1.0 - sigmoid))).astype(bf16)
    d3 = (back * activ).astype(bf16)
    keys_t = keys.T
    acc1[...] += mm(keys_t, d1)
    acc3[...] += mm(keys_t, d3)
    acc2[...] += mm(hidden.T, scaled)


def first_kernel(heads, ids, *refs):
    w1_ref, w2_ref, w3_ref, acc1, acc2, acc3, wb1, wb2, wb3, buffer, pair_sems = refs[heads:]
    groups = fetch(refs[:heads], buffer, pair_sems)

    @pl.when(pl.program_id(0) == 0)
    def _():
        wb1[...] = w1_ref[0].astype(bf16)
        wb2[...] = w2_ref[0].astype(bf16).T
        wb3[...] = w3_ref[0].astype(bf16)
        for acc in (acc1, acc2, acc3):
            acc[...] = jnp.zeros_like(acc)

    accumulate(groups, buffer, wb1, wb2, wb3, acc1, acc2, acc3)


def last_kernel(heads, ids, *refs):
    was1, was2, was3, wb1, wb2, wb3, send1, keep1, send2, keep2, send3, keep3 = refs[
        heads : heads + 12
    ]
    acc1, acc2, acc3, old1, old2, old3, sems, buffer, pair_sems = refs[heads + 12 :]
    groups = fetch(refs[:heads], buffer, pair_sems)
    loads = [
        pltpu.make_async_copy(was, old, sems.at[i])
        for i, (was, old) in enumerate(((was1, old1), (was2, old2), (was3, old3)))
    ]

    @pl.when(pl.program_id(0) == 0)
    def _():
        for load in loads:
            load.start()
        for acc in (acc1, acc2, acc3):
            acc[...] = jnp.zeros_like(acc)

    accumulate(groups, buffer, wb1, wb2, wb3, acc1, acc2, acc3)

    @pl.when(pl.program_id(0) == pl.num_programs(0) - 1)
    def _():
        half = keep1.shape[0]
        mine = pl.ds(pl.multiple_of(ids[1] * half, 16), half)
        other = pl.ds(pl.multiple_of((1 - ids[1]) * half, 16), half)
        for load, was, acc, send, keep in (
            (loads[0], old1, acc1, send1, keep1),
            (loads[2], old3, acc3, send3, keep3),
            (loads[1], old2, acc2, send2, keep2),
        ):
            load.wait()
            send[...] = (was[other, :] + acc[other, :]).astype(bf16)
            keep[...] = was[mine, :] + acc[mine, :]


def grad_call(kernel, ids, pair, others, other_specs, outs, out_specs, scratch):
    heads = len(pair)
    _, rows, width = pair[0].shape
    scratch = scratch + [
        pltpu.VMEM((heads, 2, rows, width), bf16),
        pltpu.SemaphoreType.DMA((heads,)),
    ]
    return pl.pallas_call(
        functools.partial(kernel, heads),
        grid_spec=pltpu.PrefetchScalarGridSpec(
            num_scalar_prefetch=1,
            grid=(2,),
            in_specs=[pl.BlockSpec(memory_space=pl.ANY)] * heads + other_specs,
            out_specs=out_specs,
            scratch_shapes=scratch,
        ),
        out_shape=outs,
        cost_estimate=cost(12 * heads * rows * width * width, 4 * heads * rows * width),
        compiler_params=pltpu.CompilerParams(vmem_limit_bytes=60 << 20),
    )(ids, *pair, *others)


def gradients_first(ids, pair, weights):
    width = pair[0].shape[-1]
    weight = pl.BlockSpec((1, width, width), lambda i, ids: (ids[0], 0, 0))
    full = pl.BlockSpec((width, width), lambda i, ids: (0, 0))
    outs = [jax.ShapeDtypeStruct((width, width), f32)] * 3
    outs += [jax.ShapeDtypeStruct((width, width), bf16)] * 3
    return grad_call(first_kernel, ids, pair, weights, [weight] * 3, outs, [full] * 6, [])


def gradients_last(ids, pair, carried):
    width = pair[0].shape[-1]
    rows = width // 2
    full = pl.BlockSpec((width, width), lambda i, ids: (0, 0))
    half = pl.BlockSpec((rows, width), lambda i, ids: (0, 0))
    outs = [
        jax.ShapeDtypeStruct((rows, width), bf16),
        jax.ShapeDtypeStruct((rows, width), f32),
    ] * 3
    scratch = [pltpu.VMEM((width, width), f32)] * 6 + [pltpu.SemaphoreType.DMA((3,))]
    specs = [pl.BlockSpec(memory_space=pl.ANY)] * 3 + [full] * 3
    return grad_call(last_kernel, ids, pair, carried, specs, outs, [half] * 6, scratch)


def newton_kernel(ids, own_ref, other_ref, w_ref, u_ref, g_ref):
    half = own_ref.shape[0]
    g_ref[pl.ds(pl.multiple_of(ids[1] * half, 16), half), :] = own_ref[...]
    g_ref[pl.ds(pl.multiple_of((1 - ids[1]) * half, 16), half), :] = other_ref[...]
    grad = g_ref[...].astype(f32)
    total = jnp.sqrt(jnp.sum(grad * grad))
    x = (grad / (total + frob_eps)).astype(bf16)
    for _ in range(NS_STEPS):
        square = lax.dot_general(x, x, NT, preferred_element_type=f32).astype(bf16)
        poly = (coeff_b * square.astype(f32) + coeff_c * mm(square, square)).astype(bf16)
        x = (coeff_a * x.astype(f32) + mm(poly, x)).astype(bf16)
    u_ref[...] = (w_ref[0] + step_size * x.astype(f32)).astype(bf16)


def updated(ids, halves, weight):
    rows, width = halves[0].shape
    half = pl.BlockSpec((rows, width), lambda i, ids: (0, 0))
    full = pl.BlockSpec((width, width), lambda i, ids: (0, 0))
    return pl.pallas_call(
        newton_kernel,
        grid_spec=pltpu.PrefetchScalarGridSpec(
            num_scalar_prefetch=1,
            grid=(1,),
            in_specs=[half, half, pl.BlockSpec((1, width, width), lambda i, ids: (ids[0], 0, 0))],
            out_specs=full,
            scratch_shapes=[pltpu.VMEM((width, width), bf16)],
        ),
        out_shape=jax.ShapeDtypeStruct((width, width), bf16),
        cost_estimate=cost(12 * width**3, 8 * width * width),
        compiler_params=pltpu.CompilerParams(vmem_limit_bytes=60 << 20),
    )(ids, *halves, weight)


def gate_kernel(q_ref, u1_ref, u3_ref, f_ref):
    pre1 = mm(q_ref[...], u1_ref[...])
    pre3 = mm(q_ref[...], u3_ref[...])
    f_ref[...] = (pre1 * jax.nn.sigmoid(pre1) * pre3).astype(bf16)


def output_kernel(ids, f_ref, u2_ref, *o_refs):
    out = mm(f_ref[...], u2_ref[...])
    factor = lax.rsqrt(jnp.mean(out * out, axis=-1, keepdims=True) + epsilon)
    for place, o_ref in enumerate(o_refs):

        @pl.when(pl.program_id(0) == place)
        def _():
            o_ref[...] = (out * factor).astype(bf16)


def outputs(ids, gated, weight, start, count, heads):
    tokens, width = gated.shape
    rows = tokens // heads
    return pl.pallas_call(
        output_kernel,
        grid_spec=pltpu.PrefetchScalarGridSpec(
            num_scalar_prefetch=1,
            grid=(count,),
            in_specs=[
                pl.BlockSpec((rows, width), lambda i, ids: (ids[2] ^ (start + i), 0)),
                pl.BlockSpec((width, width), lambda i, ids: (0, 0)),
            ],
            out_specs=[pl.BlockSpec((rows, width), lambda i, ids: (0, 0))] * count,
        ),
        out_shape=[jax.ShapeDtypeStruct((rows, width), bf16)] * count,
        cost_estimate=cost(2 * count * rows * width * width, 4 * count * rows * width),
        compiler_params=pltpu.CompilerParams(vmem_limit_bytes=60 << 20),
    )(ids, gated, weight)


def over_tokens(kernel, x, *weights):
    tokens, width = x.shape
    block = tokens // 4
    tile = pl.BlockSpec((block, width), lambda i: (i, 0))
    full = pl.BlockSpec((width, width), lambda i: (0, 0))
    return pl.pallas_call(
        kernel,
        grid=(tokens // block,),
        in_specs=[tile] + [full] * len(weights),
        out_specs=tile,
        out_shape=jax.ShapeDtypeStruct((tokens, width), bf16),
        cost_estimate=cost(2 * len(weights) * tokens * width * width, 4 * tokens * width),
        compiler_params=pltpu.CompilerParams(vmem_limit_bytes=60 << 20),
    )(x, *weights)


def summed(send, keep, steps):
    for place, (axis, size, bit) in enumerate(steps):
        pairs = [(i, i ^ (1 << bit)) for i in range(size)]
        came = lax.ppermute(send, axis, pairs)
        keep = keep + came.astype(f32)
        if place + 1 == len(steps):
            whole = keep.astype(bf16)
        elif place + 2 == len(steps):
            send = keep.astype(bf16)
        else:
            axis, size, bit = steps[place + 1]
            rows = keep.shape[0] // 2
            side = (lax.axis_index(axis) >> bit) & 1
            send = lax.dynamic_slice_in_dim(keep, (1 - side) * rows, rows, 0).astype(bf16)
            keep = lax.dynamic_slice_in_dim(keep, side * rows, rows, 0)
    for place, (axis, size, bit) in reversed(list(enumerate(steps[:-1]))):
        pairs = [(i, i ^ (1 << bit)) for i in range(size)]
        other = lax.ppermute(whole, axis, pairs)
        if place == 0:
            return whole, other
        first = ((lax.axis_index(axis) >> bit) & 1) == 0
        whole = jnp.concatenate(
            [jnp.where(first, whole, other), jnp.where(first, other, whole)], axis=0
        )


def per_device(
    sizes, queries, keys, values, rates, q_gain, k_gain, w_first, w_second, w_third
):
    heads = rates.shape[1]
    width = w_first.shape[1]
    exchange = functools.partial(
        lax.all_to_all, axis_name=("head", "l1", "l2"), split_axis=0, concat_axis=0, tiled=True
    )
    steps = [
        (axis, sizes[axis], bit)
        for axis in ("h2", "h1")
        for bit in range(sizes[axis].bit_length() - 1)
    ]
    axis, _, bit = steps[0]
    ids = jnp.stack([
        lax.axis_index("l1") * sizes["l2"] + lax.axis_index("l2"),
        (lax.axis_index(axis) >> bit) & 1,
        lax.axis_index(("head", "l1", "l2")),
    ]).astype(jnp.int32)

    def swap(block, k):
        pairs = [(i, i ^ k) for i in range(heads)]
        return lax.ppermute(block, ("head", "l1", "l2"), pairs)

    pairs = []
    block = keys.shape[0] // 4
    for start, count in ((0, 3), (3, 1)):
        pair = prepared_pair(ids, keys, values, rates, k_gain[None], start, count, block)
        pairs.append([pair[0]] + [swap(pair[k], k) for k in reversed(range(1, heads))])
    ready = prepared_queries(queries, q_gain[None], heads)
    query_local = exchange(ready)
    carried = gradients_first(ids, pairs[0], (w_first, w_second, w_third))
    s1, p1, s2, p2, s3, p3 = gradients_last(ids, pairs[1], carried)
    full_first = summed(s1, p1, steps)
    full_third = summed(s3, p3, steps)
    full_second = summed(s2, p2, steps)
    new_first = updated(ids, full_first, w_first)
    new_third = updated(ids, full_third, w_third)
    gated = over_tokens(gate_kernel, query_local.reshape(-1, width), new_first, new_third)
    new_second = updated(ids, full_second, w_second)
    far = heads // 2
    blocks = outputs(ids, gated, new_second, far, heads - far, heads)
    back = [swap(block, far + k) for k, block in enumerate(blocks)]
    blocks = outputs(ids, gated, new_second, 0, far, heads)
    near = [blocks[0]] + [swap(block, k) for k, block in enumerate(blocks) if k]
    return back_to_columns(ids, near + back)


def solution(mesh):
    head, ctx = mesh.shape["head"], mesh.shape["ctx"]

    def run(queries, keys, values, rates, q_gain, k_gain, w_first, w_second, w_third):
        lo = w_first.shape[0] // head
        hi = ctx // lo
        sizes = {"l2": min(lo, 2), "h2": min(hi, 2)}
        sizes["l1"] = lo // sizes["l2"]
        sizes["h1"] = hi // sizes["h2"]
        assert hi > 2 and hi * lo == ctx and ctx & (ctx - 1) == 0
        assert w_first.shape[1] % (2 * hi) == 0
        order = ("h1", "l1", "h2", "l2")
        shape = [head] + [sizes[axis] for axis in order]
        inner = Mesh(mesh.devices.reshape(shape), ("head",) + order)
        tokens = P(("head",) + order, None)
        return jax.shard_map(
            functools.partial(per_device, sizes),
            mesh=inner,
            in_specs=(tokens,) * 4 + (P(), P()) + (P("head", None, None),) * 3,
            out_specs=tokens,
            check_vma=False,
        )(queries, keys, values, rates, q_gain, k_gain, w_first, w_second, w_third)

    return run
```

```python
import functools

import jax
import jax.numpy as jnp
from jax import lax
from jax.experimental import pallas as pl
from jax.experimental.pallas import tpu as pltpu
from jax.sharding import Mesh, PartitionSpec as P


NS_STEPS = 2

epsilon = 1e-06
frob_eps = 1e-07
coeff_a = 3.4445
coeff_b = -4.775
coeff_c = 2.0315
step_size = 1.0

f32 = jnp.float32
bf16 = jnp.bfloat16
NT = (((1,), (1,)), ((), ()))


def mm(a, b):
    return jnp.dot(a, b, preferred_element_type=f32)


def cost(flops, moved):
    return pl.CostEstimate(flops=flops, bytes_accessed=moved, transcendentals=0)


def normalized(x_ref, gain_ref, out_ref, place):
    heads, width = out_ref.shape[0], out_ref.shape[-1]
    wide = x_ref[...].astype(f32)
    factor = lax.rsqrt(jnp.mean(wide * wide, axis=-1, keepdims=True) + epsilon)
    for head in range(heads):
        cols = slice(head * width, (head + 1) * width)
        out_ref[place(head)] = (
            x_ref[:, cols].astype(f32) * factor * gain_ref[:, cols]
        ).astype(bf16)


def query_kernel(x_ref, gain_ref, out_ref):
    normalized(x_ref, gain_ref, out_ref, lambda head: head)


def pair_kernel(ids, k_ref, v_ref, rate_ref, gain_ref, *out_refs):
    width = out_refs[0].shape[-1]
    wide = k_ref[...].astype(f32)
    factor = lax.rsqrt(jnp.mean(wide * wide, axis=-1, keepdims=True) + epsilon)
    rates = rate_ref[...].astype(f32)
    lane = lax.broadcasted_iota(jnp.int32, rates.shape, 1)
    for k, out_ref in enumerate(out_refs):
        head = ids[2] ^ k
        cols = pl.ds(pl.multiple_of(head * width, 128), width)
        out_ref[0] = (k_ref[:, cols].astype(f32) * factor * gain_ref[:, cols]).astype(bf16)
        rate = jnp.sum(jnp.where(lane == head, rates, 0.0), axis=1, keepdims=True)
        out_ref[1] = (v_ref[:, cols].astype(f32) * rate).astype(bf16)


def prepared_queries(x, gain, heads):
    rows, model = x.shape
    width = model // heads
    block = rows // 4 if rows % 64 == 0 else rows
    return pl.pallas_call(
        query_kernel,
        grid=(rows // block,),
        in_specs=[
            pl.BlockSpec((block, model), lambda i: (i, 0)),
            pl.BlockSpec((1, model), lambda i: (0, 0)),
        ],
        out_specs=pl.BlockSpec((heads, block, width), lambda i: (0, i, 0)),
        out_shape=jax.ShapeDtypeStruct((heads, rows, width), bf16),
        cost_estimate=cost(8 * rows * model, 4 * rows * model),
    )(x, gain)


def prepared_pair(ids, keys, values, rates, gain, first, steps, block):
    heads = rates.shape[1]
    model = keys.shape[1]
    rows = block * steps
    width = model // heads
    tile = pl.BlockSpec((block, model), lambda i, ids: (first + i, 0))
    return pl.pallas_call(
        pair_kernel,
        grid_spec=pltpu.PrefetchScalarGridSpec(
            num_scalar_prefetch=1,
            grid=(steps,),
            in_specs=[
                tile,
                tile,
                pl.BlockSpec((block, heads), lambda i, ids: (first + i, 0)),
                pl.BlockSpec((1, model), lambda i, ids: (0, 0)),
            ],
            out_specs=[pl.BlockSpec((2, block, width), lambda i, ids: (0, i, 0))] * heads,
        ),
        out_shape=[jax.ShapeDtypeStruct((2, rows, width), bf16)] * heads,
        cost_estimate=cost(12 * rows * model, 8 * rows * model),
    )(ids, keys, values, rates, gain)


def back_to_columns(ids, blocks):
    rows, width = blocks[0].shape
    heads = len(blocks)

    def kernel(ids, *refs):
        out_ref = refs[-1]
        for k, ref in enumerate(refs[:-1]):
            start = pl.multiple_of((ids[2] ^ k) * width, 128)
            out_ref[:, pl.ds(start, width)] = ref[...]

    block = rows // 4
    return pl.pallas_call(
        kernel,
        grid_spec=pltpu.PrefetchScalarGridSpec(
            num_scalar_prefetch=1,
            grid=(rows // block,),
            in_specs=[pl.BlockSpec((block, width), lambda i, ids: (i, 0))] * heads,
            out_specs=pl.BlockSpec((block, heads * width), lambda i, ids: (i, 0)),
        ),
        out_shape=jax.ShapeDtypeStruct((rows, heads * width), bf16),
        cost_estimate=cost(rows * heads * width, 4 * rows * heads * width),
    )(ids, *blocks)


def fetch(pair_refs, buffer, sems):
    loads = [
        pltpu.make_async_copy(ref, buffer.at[i], sems.at[i]) for i, ref in enumerate(pair_refs)
    ]
    half = len(loads) // 2

    @pl.when(pl.program_id(0) == 0)
    def _():
        for load in loads:
            load.start()

    return loads[:half], loads[half:]


def accumulate(groups, buffer, wb1, wb2, wb3, acc1, acc2, acc3):
    for step, group in enumerate(groups):

        @pl.when(pl.program_id(0) == step)
        def _():
            for load in group:
                load.wait()

    sources, rows, width = buffer.shape[0] // 2, buffer.shape[2], buffer.shape[3]
    now = pl.ds(pl.program_id(0) * sources, sources)
    keys = buffer[now, 0].reshape(sources * rows, width)
    scaled = buffer[now, 1].reshape(sources * rows, width)
    pre1 = mm(keys, wb1[...])
    pre3 = mm(keys, wb3[...])
    sigmoid = jax.nn.sigmoid(pre1)
    activ = pre1 * sigmoid
    hidden = (activ * pre3).astype(bf16)
    back = mm(scaled, wb2[...])
    d1 = (back * pre3 * sigmoid * (1.0 + pre1 * (1.0 - sigmoid))).astype(bf16)
    d3 = (back * activ).astype(bf16)
    keys_t = keys.T
    acc1[...] += mm(keys_t, d1)
    acc3[...] += mm(keys_t, d3)
    acc2[...] += mm(hidden.T, scaled)


def first_kernel(heads, ids, *refs):
    w1_ref, w2_ref, w3_ref, acc1, acc2, acc3, wb1, wb2, wb3, buffer, pair_sems = refs[heads:]
    groups = fetch(refs[:heads], buffer, pair_sems)

    @pl.when(pl.program_id(0) == 0)
    def _():
        wb1[...] = w1_ref[0].astype(bf16)
        wb2[...] = w2_ref[0].astype(bf16).T
        wb3[...] = w3_ref[0].astype(bf16)
        for acc in (acc1, acc2, acc3):
            acc[...] = jnp.zeros_like(acc)

    accumulate(groups, buffer, wb1, wb2, wb3, acc1, acc2, acc3)


def last_kernel(heads, ids, *refs):
    was1, was2, was3, wb1, wb2, wb3, send1, keep1, send2, keep2, send3, keep3 = refs[
        heads : heads + 12
    ]
    acc1, acc2, acc3, old1, old2, old3, sems, buffer, pair_sems = refs[heads + 12 :]
    groups = fetch(refs[:heads], buffer, pair_sems)
    loads = [
        pltpu.make_async_copy(was, old, sems.at[i])
        for i, (was, old) in enumerate(((was1, old1), (was2, old2), (was3, old3)))
    ]

    @pl.when(pl.program_id(0) == 0)
    def _():
        for load in loads:
            load.start()
        for acc in (acc1, acc2, acc3):
            acc[...] = jnp.zeros_like(acc)

    accumulate(groups, buffer, wb1, wb2, wb3, acc1, acc2, acc3)

    @pl.when(pl.program_id(0) == pl.num_programs(0) - 1)
    def _():
        half = keep1.shape[0]
        mine = pl.ds(pl.multiple_of(ids[1] * half, 16), half)
        other = pl.ds(pl.multiple_of((1 - ids[1]) * half, 16), half)
        for load, was, acc, send, keep in (
            (loads[0], old1, acc1, send1, keep1),
            (loads[2], old3, acc3, send3, keep3),
            (loads[1], old2, acc2, send2, keep2),
        ):
            load.wait()
            send[...] = (was[other, :] + acc[other, :]).astype(bf16)
            keep[...] = was[mine, :] + acc[mine, :]


def grad_call(kernel, ids, pair, others, other_specs, outs, out_specs, scratch):
    heads = len(pair)
    _, rows, width = pair[0].shape
    scratch = scratch + [
        pltpu.VMEM((heads, 2, rows, width), bf16),
        pltpu.SemaphoreType.DMA((heads,)),
    ]
    return pl.pallas_call(
        functools.partial(kernel, heads),
        grid_spec=pltpu.PrefetchScalarGridSpec(
            num_scalar_prefetch=1,
            grid=(2,),
            in_specs=[pl.BlockSpec(memory_space=pl.ANY)] * heads + other_specs,
            out_specs=out_specs,
            scratch_shapes=scratch,
        ),
        out_shape=outs,
        cost_estimate=cost(12 * heads * rows * width * width, 4 * heads * rows * width),
        compiler_params=pltpu.CompilerParams(vmem_limit_bytes=60 << 20),
    )(ids, *pair, *others)


def gradients_first(ids, pair, weights):
    width = pair[0].shape[-1]
    weight = pl.BlockSpec((1, width, width), lambda i, ids: (ids[0], 0, 0))
    full = pl.BlockSpec((width, width), lambda i, ids: (0, 0))
    outs = [jax.ShapeDtypeStruct((width, width), f32)] * 3
    outs += [jax.ShapeDtypeStruct((width, width), bf16)] * 3
    return grad_call(first_kernel, ids, pair, weights, [weight] * 3, outs, [full] * 6, [])


def gradients_last(ids, pair, carried):
    width = pair[0].shape[-1]
    rows = width // 2
    full = pl.BlockSpec((width, width), lambda i, ids: (0, 0))
    half = pl.BlockSpec((rows, width), lambda i, ids: (0, 0))
    outs = [
        jax.ShapeDtypeStruct((rows, width), bf16),
        jax.ShapeDtypeStruct((rows, width), f32),
    ] * 3
    scratch = [pltpu.VMEM((width, width), f32)] * 6 + [pltpu.SemaphoreType.DMA((3,))]
    specs = [pl.BlockSpec(memory_space=pl.ANY)] * 3 + [full] * 3
    return grad_call(last_kernel, ids, pair, carried, specs, outs, [half] * 6, scratch)


def newton_kernel(ids, own_ref, other_ref, w_ref, u_ref, g_ref):
    half = own_ref.shape[0]
    g_ref[pl.ds(pl.multiple_of(ids[1] * half, 16), half), :] = own_ref[...]
    g_ref[pl.ds(pl.multiple_of((1 - ids[1]) * half, 16), half), :] = other_ref[...]
    grad = g_ref[...].astype(f32)
    total = jnp.sqrt(jnp.sum(grad * grad))
    x = (grad / (total + frob_eps)).astype(bf16)
    for _ in range(NS_STEPS):
        square = lax.dot_general(x, x, NT, preferred_element_type=f32).astype(bf16)
        poly = (coeff_b * square.astype(f32) + coeff_c * mm(square, square)).astype(bf16)
        x = (coeff_a * x.astype(f32) + mm(poly, x)).astype(bf16)
    u_ref[...] = (w_ref[0] + step_size * x.astype(f32)).astype(bf16)


def updated(ids, halves, weight):
    rows, width = halves[0].shape
    half = pl.BlockSpec((rows, width), lambda i, ids: (0, 0))
    full = pl.BlockSpec((width, width), lambda i, ids: (0, 0))
    return pl.pallas_call(
        newton_kernel,
        grid_spec=pltpu.PrefetchScalarGridSpec(
            num_scalar_prefetch=1,
            grid=(1,),
            in_specs=[half, half, pl.BlockSpec((1, width, width), lambda i, ids: (ids[0], 0, 0))],
            out_specs=full,
            scratch_shapes=[pltpu.VMEM((width, width), bf16)],
        ),
        out_shape=jax.ShapeDtypeStruct((width, width), bf16),
        cost_estimate=cost(12 * width**3, 8 * width * width),
        compiler_params=pltpu.CompilerParams(vmem_limit_bytes=60 << 20),
    )(ids, *halves, weight)


def gate_kernel(q_ref, u1_ref, u3_ref, f_ref):
    pre1 = mm(q_ref[...], u1_ref[...])
    pre3 = mm(q_ref[...], u3_ref[...])
    f_ref[...] = (pre1 * jax.nn.sigmoid(pre1) * pre3).astype(bf16)


def output_kernel(ids, f_ref, u2_ref, *o_refs):
    out = mm(f_ref[...], u2_ref[...])
    factor = lax.rsqrt(jnp.mean(out * out, axis=-1, keepdims=True) + epsilon)
    for place, o_ref in enumerate(o_refs):

        @pl.when(pl.program_id(0) == place)
        def _():
            o_ref[...] = (out * factor).astype(bf16)


def outputs(ids, gated, weight, bit, heads):
    tokens, width = gated.shape
    low, count = heads // 4, heads // 2
    rows = tokens // heads
    return pl.pallas_call(
        output_kernel,
        grid_spec=pltpu.PrefetchScalarGridSpec(
            num_scalar_prefetch=1,
            grid=(count,),
            in_specs=[
                pl.BlockSpec((rows, width), lambda i, ids: (ids[2] ^ (i // low * 2 * low + bit * low + i % low), 0)),
                pl.BlockSpec((width, width), lambda i, ids: (0, 0)),
            ],
            out_specs=[pl.BlockSpec((rows, width), lambda i, ids: (0, 0))] * count,
        ),
        out_shape=[jax.ShapeDtypeStruct((rows, width), bf16)] * count,
        cost_estimate=cost(2 * count * rows * width * width, 4 * count * rows * width),
        compiler_params=pltpu.CompilerParams(vmem_limit_bytes=60 << 20),
    )(ids, gated, weight)


def over_tokens(kernel, x, *weights):
    tokens, width = x.shape
    block = tokens // 4
    tile = pl.BlockSpec((block, width), lambda i: (i, 0))
    full = pl.BlockSpec((width, width), lambda i: (0, 0))
    return pl.pallas_call(
        kernel,
        grid=(tokens // block,),
        in_specs=[tile] + [full] * len(weights),
        out_specs=tile,
        out_shape=jax.ShapeDtypeStruct((tokens, width), bf16),
        cost_estimate=cost(2 * len(weights) * tokens * width * width, 4 * tokens * width),
        compiler_params=pltpu.CompilerParams(vmem_limit_bytes=60 << 20),
    )(x, *weights)


def summed(send, keep, steps):
    for place, (axis, size, bit) in enumerate(steps):
        pairs = [(i, i ^ (1 << bit)) for i in range(size)]
        came = lax.ppermute(send, axis, pairs)
        keep = keep + came.astype(f32)
        if place + 1 == len(steps):
            whole = keep.astype(bf16)
        elif place + 2 == len(steps):
            send = keep.astype(bf16)
        else:
            axis, size, bit = steps[place + 1]
            rows = keep.shape[0] // 2
            side = (lax.axis_index(axis) >> bit) & 1
            send = lax.dynamic_slice_in_dim(keep, (1 - side) * rows, rows, 0).astype(bf16)
            keep = lax.dynamic_slice_in_dim(keep, side * rows, rows, 0)
    for place, (axis, size, bit) in reversed(list(enumerate(steps[:-1]))):
        pairs = [(i, i ^ (1 << bit)) for i in range(size)]
        other = lax.ppermute(whole, axis, pairs)
        if place == 0:
            return whole, other
        first = ((lax.axis_index(axis) >> bit) & 1) == 0
        whole = jnp.concatenate(
            [jnp.where(first, whole, other), jnp.where(first, other, whole)], axis=0
        )


def per_device(
    sizes, queries, keys, values, rates, q_gain, k_gain, w_first, w_second, w_third
):
    heads = rates.shape[1]
    width = w_first.shape[1]
    exchange = functools.partial(
        lax.all_to_all, axis_name=("head", "l1", "l2"), split_axis=0, concat_axis=0, tiled=True
    )
    steps = [
        (axis, sizes[axis], bit)
        for axis in ("h2", "h1")
        for bit in range(sizes[axis].bit_length() - 1)
    ]
    axis, _, bit = steps[0]
    ids = jnp.stack([
        lax.axis_index("l1") * sizes["l2"] + lax.axis_index("l2"),
        (lax.axis_index(axis) >> bit) & 1,
        lax.axis_index(("head", "l1", "l2")),
    ]).astype(jnp.int32)

    def swap(block, k):
        pairs = [(i, i ^ k) for i in range(heads)]
        return lax.ppermute(block, ("head", "l1", "l2"), pairs)

    pairs = []
    block = keys.shape[0] // 4
    for start, count in ((0, 3), (3, 1)):
        pair = prepared_pair(ids, keys, values, rates, k_gain[None], start, count, block)
        pairs.append([pair[0]] + [swap(pair[k], k) for k in reversed(range(1, heads))])
    ready = prepared_queries(queries, q_gain[None], heads)
    query_local = exchange(ready)
    carried = gradients_first(ids, pairs[0], (w_first, w_second, w_third))
    s1, p1, s2, p2, s3, p3 = gradients_last(ids, pairs[1], carried)
    full_first = summed(s1, p1, steps)
    full_third = summed(s3, p3, steps)
    full_second = summed(s2, p2, steps)
    new_first = updated(ids, full_first, w_first)
    new_third = updated(ids, full_third, w_third)
    gated = over_tokens(gate_kernel, query_local.reshape(-1, width), new_first, new_third)
    new_second = updated(ids, full_second, w_second)
    ready = [None] * heads
    for bit in (1, 0):
        blocks = outputs(ids, gated, new_second, bit, heads)
        places = [k for k in range(heads) if (k // (heads // 4)) % 2 == bit]
        for k, block in reversed(list(zip(places, blocks))):
            ready[k] = swap(block, k) if k else block
    return back_to_columns(ids, ready)


def solution(mesh):
    head, ctx = mesh.shape["head"], mesh.shape["ctx"]

    def run(queries, keys, values, rates, q_gain, k_gain, w_first, w_second, w_third):
        lo = w_first.shape[0] // head
        hi = ctx // lo
        sizes = {"l2": min(lo, 2), "h2": min(hi, 2)}
        sizes["l1"] = lo // sizes["l2"]
        sizes["h1"] = hi // sizes["h2"]
        assert hi > 2 and hi * lo == ctx and ctx & (ctx - 1) == 0
        assert w_first.shape[1] % (2 * hi) == 0
        order = ("h1", "l1", "h2", "l2")
        shape = [head] + [sizes[axis] for axis in order]
        inner = Mesh(mesh.devices.reshape(shape), ("head",) + order)
        tokens = P(("head",) + order, None)
        return jax.shard_map(
            functools.partial(per_device, sizes),
            mesh=inner,
            in_specs=(tokens,) * 4 + (P(), P()) + (P("head", None, None),) * 3,
            out_specs=tokens,
            check_vma=False,
        )(queries, keys, values, rates, q_gain, k_gain, w_first, w_second, w_third)

    return run
```
